256 devices in a mesh: rows: 64 (over z, y, core), mem: 4 (over x).
Axes of the slice: x: 4, y: 4, z: 8, core: 2. Of those that a mesh axis runs over, the one named last changes fastest.
Arguments:
- control: bfloat16 [16, 32, 2, 512, 512], P('mem', None, None, 'rows'), may hold values from -6 to 6
- vert_root: float32 [32, 32], replicated, may hold values from -1 to 1
- loc_spec: float32 [512], replicated, may hold values from 0.1 to 1
- legendre: bfloat16 [512, 512, 768], P('rows'), as said below
- wave_table: int32 [512], replicated, may hold values from 0 to 511, as said below
- lat_order: int32 [768], replicated, may hold values from 0 to 767, each once
- perturb: bfloat16 [768, 16, 32, 1536], P('rows', None, 'mem'), may hold values from -3 to 3
Outputs:
- increment: bfloat16 [768, 32, 1536], P('rows', 'mem')
The draws below stay inside these ranges and needn't reach their ends.
Inputs may be any that keep to these rules, and one draw needn't show every extreme that they name: `wave_table`: every zonal wavenumber 0 to 511 sits in exactly one slot; the slots held by one index of rows are pairs m and 511 - m. legendre[s, n, t] is zero where n < wave_table[s]. `lat_order`: a permutation.
All inputs are finite; a program needn't handle non-finite values.
Results may differ from the reference program's by a relative error of at most 0.0085.
Values may be sent and summed in bfloat16 or wider, within the bound.
No kernel may reach another device: no remote copies, remote signals or barrier semaphores. Data moves between devices by JAX's collectives and lax.ppermute only.
A program may use at most 128 MiB of HBM per device.

```python
import math
import jax
import jax.numpy as jnp
from jax import lax

NM = 512
NT = 512
NLAT = 768
NLON = 1536
MEMBERS = 16
LEV = 32
N_ROWS = 64


def pair_table(key):
    subkey = jax.random.fold_in(key, 7)
    permuted = jax.random.permutation(subkey, NM // 2).astype(jnp.int32)
    lower_half = permuted.reshape(N_ROWS, NM // (2 * N_ROWS))
    return jnp.concatenate([lower_half, NM - 1 - lower_half], axis=1).reshape(NM).astype(jnp.int32)


def draw_wave_table(key, part):
    return pair_table(key)


def draw_legendre(key, part):
    table = pair_table(key)
    subkey = jax.random.fold_in(key, 11)
    values = jax.random.normal(subkey, (NM, NT, NLAT), jnp.float32)
    totals = jnp.arange(NT, dtype=jnp.int32)
    triangle = (totals[None, :] >= table[:, None]).astype(jnp.float32)
    factor = (4.0 * NM * NT) ** (-0.5)
    return (values * factor * triangle[:, :, None]).astype(jnp.bfloat16)


def block_levels(key, extent, split, low, top_value):
    level = 1.0
    for dim, shards_of in split:
        draws = jax.random.uniform(jax.random.fold_in(jax.random.fold_in(key, 6), dim), (shards_of,), jnp.float32, low / len(split), top_value / len(split))
        level = level * jnp.repeat(jnp.exp(draws), extent[dim] // shards_of).reshape((-1,) + (1,) * (len(extent) - 1 - dim))
    return level


def noise(rng, dims, spread, reach, pieces=(), held_as=jnp.bfloat16):
    gain = block_levels(rng, dims, pieces, -0.22, 0.18) if pieces else 1.0
    values = jax.random.normal(rng, dims, jnp.float32) * spread * gain
    return jnp.minimum(jnp.maximum(values, -reach), reach).astype(held_as)


def setup_inputs(seed: int = 0) -> dict:
    key_list = jax.random.split(jax.random.key(seed), 8)
    control = noise(key_list[0], (MEMBERS, LEV, 2, NM, NT), 1.0, 6.0, ((0, 4), (3, 64)))
    vert_root = noise(key_list[1], (LEV, LEV), LEV ** -0.5, 1.0, (), jnp.float32)
    loc_spec = jnp.clip(jnp.exp(jax.random.uniform(key_list[2], (NT,), jnp.float32, math.log(0.1), math.log(1.0))), 0.1, 1.0)
    legendre = draw_legendre(jax.random.fold_in(key_list[7], 71), 0)
    wave_table = draw_wave_table(jax.random.fold_in(key_list[7], 71), 0)
    lat_order = jax.random.permutation(key_list[5], NLAT).astype(jnp.int32)
    perturb = noise(key_list[6], (NLAT, MEMBERS, LEV, NLON), 0.5, 3.0, ((0, 64), (2, 4)))
    return {"control": control, "vert_root": vert_root, "loc_spec": loc_spec, "legendre": legendre, "wave_table": wave_table, "lat_order": lat_order, "perturb": perturb}


def make_basis(wave_table, lon_count):
    longitude = lax.iota(jnp.int32, lon_count)
    phases = (wave_table[:, None] * longitude[None, :]) % lon_count
    angles = phases.astype(jnp.float32) * (2.0 * math.pi / lon_count)
    weights = jnp.where(wave_table == 0, 1.0, 2.0).astype(jnp.float32)[:, None]
    return jnp.stack([weights * jnp.cos(angles), -weights * jnp.sin(angles)]).astype(jnp.bfloat16)


def reference(control, vert_root, loc_spec, legendre, wave_table, lat_order, perturb):
    scaled = control.astype(jnp.float32) * loc_spec
    spectra = jnp.einsum('lv,kvrsn->klrsn', vert_root, scaled, precision=lax.Precision.HIGHEST).astype(jnp.bfloat16)
    zonal_basis = make_basis(wave_table, NLON).astype(jnp.float32)
    legendre_wide = legendre.astype(jnp.float32)

    def one_level(level_index):
        level_spec = lax.dynamic_index_in_dim(spectra, level_index, 1, keepdims=False).astype(jnp.float32)
        fourier = jnp.einsum('snt,krsn->strk', legendre_wide, level_spec, precision=lax.Precision.HIGHEST).astype(jnp.bfloat16)
        fourier = jnp.take(fourier, lat_order, axis=1).astype(jnp.float32)
        fields = jnp.einsum('sjrk,rsx->jkx', fourier, zonal_basis, precision=lax.Precision.HIGHEST).astype(jnp.bfloat16)
        member_ptb = lax.dynamic_index_in_dim(perturb, level_index, 2, keepdims=False).astype(jnp.float32)
        return jnp.sum(fields.astype(jnp.float32) * member_ptb, axis=1).astype(jnp.bfloat16)

    stacked = lax.map(one_level, jnp.arange(LEV, dtype=jnp.int32))
    return jnp.transpose(stacked, (1, 0, 2))
```

```python
import math

import jax
import jax.numpy as jnp
from jax import lax
from jax.experimental import pallas as pl
from jax.experimental.pallas import tpu as pltpu
from jax.sharding import PartitionSpec as P

F32 = jnp.float32
BF16 = jnp.bfloat16
SUB = 4
PITCH = 200


def dot(a, b, dims):
    return lax.dot_general(a, b, (dims, ((), ())), preferred_element_type=F32)


def front_kernel(root_ref, loc_ref, lat_ref, ctrl_ref, leg_ref, out_ref, spec_scr, perm_scr, stage_scr):
    slot = pl.program_id(0)
    slots = pl.num_programs(0)
    members = ctrl_ref.shape[0]
    lats = perm_scr.shape[0]
    groups = lats // SUB

    @pl.when(slot == 0)
    def _():
        lat_col = jnp.transpose(jnp.broadcast_to(lat_ref[...].astype(F32), (8, lats)))[:, :1]
        cols = lax.broadcasted_iota(jnp.int32, (lats, lats), 1).astype(F32)
        perm_scr[...] = jnp.where(cols == lat_col, 1.0, 0.0).astype(BF16)
        root = root_ref[...]
        high = root.astype(BF16)
        low = (root - high.astype(F32)).astype(BF16)
        rows = lax.broadcasted_iota(jnp.int32, (512, 32), 0)
        lanes = lax.broadcasted_iota(jnp.int32, (512, 32), 1)
        pick_l = jnp.where(rows % 32 == lanes, 1.0, 0.0).astype(BF16)
        rows = lax.broadcasted_iota(jnp.int32, (32, 512), 0)
        lanes = lax.broadcasted_iota(jnp.int32, (32, 512), 1)
        pick_v = jnp.where(rows == lanes // 16, 1.0, 0.0).astype(BF16)
        rows = lax.broadcasted_iota(jnp.int32, (512, 512), 0)
        lanes = lax.broadcasted_iota(jnp.int32, (512, 512), 1)
        same = rows // 32 == lanes % 16
        mixes = []
        for part in (high, low):
            spread = dot(pick_l, part, ((1,), (0,))).astype(BF16)
            spread = dot(spread, pick_v, ((1,), (0,)))
            mixes.append(jnp.where(same, spread, 0.0).astype(BF16))
        for k in range(members):
            coefs = ctrl_ref[k].reshape(512, 512)
            mixed = dot(mixes[0], coefs, ((1,), (0,))) + dot(mixes[1], coefs, ((1,), (0,)))
            mixed = mixed * loc_ref[...]
            for r in range(2):
                for s in range(8):
                    for q in range(4):
                        src = (r * 8 + s) * 32 + q * 8
                        spec_scr[s, pl.ds(q * 64 + r * 32 + k * 8, 8), :] = mixed[src:src + 8]

    spec = spec_scr[slot].astype(BF16)
    fourier = dot(spec, leg_ref[0], ((1,), (0,))).astype(BF16)
    sorted_rows = dot(perm_scr[...], fourier, ((1,), (1,)))
    lane_group = lax.broadcasted_iota(jnp.int32, (groups, 128), 1) // 32
    base = pl.multiple_of(slot * PITCH, 8)
    for half in range(2):
        parts = [sorted_rows[a * groups:(a + 1) * groups, half * 128:(half + 1) * 128] for a in range(SUB)]
        turned = []
        for d in range(SUB):
            mix = parts[d]
            for p in range(1, SUB):
                mix = jnp.where(lane_group == p, parts[(p + d) % SUB], mix)
            turned.append(pltpu.roll(mix, 32 * d, 1) if d else mix)
        for q in range(4):
            piece = turned[(0 - q) % SUB]
            for a in range(1, SUB):
                piece = jnp.where(lane_group == a, turned[(a - q) % SUB], piece)
            stage_scr[half * 4 + q, pl.ds(base, groups), :] = piece

    @pl.when(slot == slots - 1)
    def _():
        def emit(row, carry):
            for third in range(3):
                for q in range(4):
                    tiles = [stage_scr[q * 2 + r, pl.ds(row * 3 + third, 8, stride=PITCH), :] for r in range(2)]
                    out_ref[row, q, third] = jnp.concatenate(tiles, axis=0).astype(BF16)
            return carry
        lax.fori_loop(0, 64, emit, 0)


def front(control, vert_root, loc_spec, legendre, lat_order):
    members, levels, _, slots, waves = control.shape
    lats = legendre.shape[2]
    ctrl = control.reshape(members, levels, 2 * slots, waves)
    lat_row = lat_order.reshape(lats // SUB, SUB).T.reshape(1, lats)
    return pl.pallas_call(
        front_kernel,
        grid=(slots,),
        in_specs=[
            pl.BlockSpec((levels, levels), lambda s: (0, 0)),
            pl.BlockSpec((1, waves), lambda s: (0, 0)),
            pl.BlockSpec((1, lats), lambda s: (0, 0)),
            pl.BlockSpec(ctrl.shape, lambda s: (0, 0, 0, 0)),
            pl.BlockSpec((1, waves, lats), lambda s: (s, 0, 0)),
        ],
        out_specs=pl.BlockSpec((64, 4, 3, 16, 128), lambda s: (0, 0, 0, 0, 0)),
        out_shape=jax.ShapeDtypeStruct((64, 4, 3, 16, 128), BF16),
        scratch_shapes=[
            pltpu.VMEM((slots, 256, waves), F32),
            pltpu.VMEM((lats, lats), BF16),
            pltpu.VMEM((8, slots * PITCH, 128), F32),
        ],
        compiler_params=pltpu.CompilerParams(vmem_limit_bytes=60 * 1024 * 1024),
        name="front",
    )(vert_root, loc_spec.reshape(1, waves), lat_row, ctrl, legendre)


def make_basis(wave_table, lon_count):
    waves = wave_table.reshape(-1, 1, 8, 1)
    longitude = lax.iota(jnp.int32, lon_count)
    phases = waves * longitude % lon_count
    angles = phases.astype(F32) * (2.0 * math.pi / lon_count)
    weights = jnp.where(waves == 0, 1.0, 2.0).astype(F32)
    pair = jnp.concatenate([weights * jnp.cos(angles), -weights * jnp.sin(angles)], axis=1)
    return pair.astype(BF16).reshape(-1, lon_count)


COLS = 256


def back_kernel(recv_ref, basis_ref, ptb_ref, out_ref, turn_scr):
    for q in range(4):
        coefs = recv_ref[:, q, 0].reshape(1024, 128)
        turn_scr[pl.ds(q * 128, 128), :] = jnp.transpose(coefs)
    for c in range(basis_ref.shape[1] // COLS):
        cols = pl.ds(c * COLS, COLS)
        field = dot(turn_scr[...], basis_ref[:, cols], ((1,), (0,))).astype(BF16).astype(F32)
        field = field.reshape(4, SUB, 4, 8, COLS)
        for a in range(SUB):
            total = None
            for q in range(4):
                for k in range(4):
                    term = field[q, a, k] * ptb_ref[a, q * 4 + k, :, cols].astype(F32)
                    total = term if total is None else total + term
            out_ref[a, :, cols] = total.astype(BF16)


def back(recv, basis, perturb):
    lats, members, levels, lons = perturb.shape
    return pl.pallas_call(
        back_kernel,
        grid=(3,),
        in_specs=[
            pl.BlockSpec((64, 4, 1, 16, 128), lambda j: (0, 0, j, 0, 0)),
            pl.BlockSpec((1024, lons), lambda j: (0, 0)),
            pl.BlockSpec((SUB, members, levels, lons), lambda j: (j, 0, 0, 0)),
        ],
        out_specs=pl.BlockSpec((SUB, levels, lons), lambda j: (j, 0, 0)),
        out_shape=jax.ShapeDtypeStruct((lats, levels, lons), BF16),
        scratch_shapes=[pltpu.VMEM((512, 1024), BF16)],
        compiler_params=pltpu.CompilerParams(vmem_limit_bytes=60 * 1024 * 1024),
        name="back",
    )(recv, basis, perturb)


def shards(control, vert_root, loc_spec, legendre, wave_table, lat_order, perturb):
    send = front(control, vert_root, loc_spec, legendre, lat_order)
    recv = lax.all_to_all(send.reshape(256, 3, 16, 128), ("rows", "mem"), 0, 0, tiled=True)
    basis = make_basis(wave_table, perturb.shape[3])
    return back(recv.reshape(64, 4, 3, 16, 128), basis, perturb)


def solution(mesh):
    return jax.shard_map(
        shards,
        mesh=mesh,
        in_specs=(
            P("mem", None, None, "rows", None),
            P(),
            P(),
            P("rows", None, None),
            P(),
            P(),
            P("rows", None, "mem", None),
        ),
        out_specs=P("rows", "mem", None),
        check_vma=False,
    )
```

```python
import math

import jax
import jax.numpy as jnp
from jax import lax
from jax.experimental import pallas as pl
from jax.experimental.pallas import tpu as pltpu
from jax.sharding import PartitionSpec as P

F32 = jnp.float32
BF16 = jnp.bfloat16
SUB = 4
UNROLL = 2
PITCH = 200


def dot(a, b, dims):
    return lax.dot_general(a, b, (dims, ((), ())), preferred_element_type=F32)


def front_kernel(root_ref, loc_ref, lat_ref, ctrl_hbm, leg_hbm, out_hbm,
                 ctrl_ref, leg_ref, spec_scr, mix_scr, perm_scr, stage_scr, out_ref, ctrl_sem, leg_sem, out_sem):
    members = ctrl_ref.shape[0]
    slots, waves, lats = leg_ref.shape
    groups = lats // SUB
    dests = out_ref.shape[0]
    ctrl_in = [pltpu.make_async_copy(ctrl_hbm.at[k], ctrl_ref.at[k], ctrl_sem.at[k]) for k in range(members)]
    leg_in = [pltpu.make_async_copy(leg_hbm.at[s], leg_ref.at[s], leg_sem.at[s]) for s in range(slots)]
    for copy in ctrl_in + leg_in:
        copy.start()

    rows = lax.broadcasted_iota(jnp.int32, (32, 512), 0)
    lanes = lax.broadcasted_iota(jnp.int32, (32, 512), 1)
    pick_v = jnp.where(rows == lanes // 16, 1.0, 0.0).astype(BF16)
    spread = dot(root_ref[...].astype(BF16), pick_v, ((1,), (0,)))

    def mix_rows(h, carry):
        mix_scr[pl.ds(pl.multiple_of(h * 32, 32), 32), :] = jnp.where(lanes % 16 == h, spread, 0.0).astype(BF16)
        return carry

    lax.fori_loop(0, 16, mix_rows, 0)

    lat_row = jnp.broadcast_to(lat_ref[...].reshape(1, lats).astype(F32), (128, lats))
    stage_scr[0, pl.ds(0, lats), :] = jnp.transpose(lat_row)
    cols = lax.broadcasted_iota(jnp.int32, (groups, 128), 1).astype(F32)

    def pick_rows(a, carry):
        wanted = stage_scr[0, pl.ds(a, groups, stride=SUB), :]
        rows = pl.ds(pl.multiple_of(a * groups, 64), groups)
        for c in range(lats // 128):
            hit = jnp.where(cols + 128.0 * c == wanted, 1.0, 0.0).astype(BF16)
            perm_scr[rows, pl.ds(c * 128, 128)] = hit
        return carry

    lax.fori_loop(0, SUB, pick_rows, 0)

    def mix_member(k, carry):
        pltpu.make_async_copy(ctrl_hbm.at[k], ctrl_ref.at[k], ctrl_sem.at[k]).wait()
        mixed = dot(mix_scr[...], ctrl_ref[k].reshape(512, waves), ((1,), (0,))) * loc_ref[...]
        for r in range(2):
            for s in range(slots):
                for q in range(4):
                    src = (r * slots + s) * 32 + q * 8
                    rows = pl.ds(pl.multiple_of(q * 64 + r * 32 + k * 8, 8), 8)
                    spec_scr[s, rows, :] = mixed[src:src + 8]
        return carry

    lax.fori_loop(0, members, mix_member, 0)

    def one_slot(slot):
        spec = spec_scr[slot].astype(BF16)
        fourier = dot(spec, leg_ref[slot], ((1,), (0,))).astype(BF16)
        sorted_rows = dot(perm_scr[...], fourier, ((1,), (1,)))
        lane_group = lax.broadcasted_iota(jnp.int32, (groups, 128), 1) // 32
        for half in range(2):
            parts = [sorted_rows[a * groups:(a + 1) * groups, half * 128:(half + 1) * 128] for a in range(SUB)]
            turned = []
            for d in range(SUB):
                piece = parts[d]
                for p in range(1, SUB):
                    piece = jnp.where(lane_group == p, parts[(p + d) % SUB], piece)
                turned.append(pltpu.roll(piece, 32 * d, 1) if d else piece)
            for q in range(4):
                piece = turned[(0 - q) % SUB]
                for a in range(1, SUB):
                    piece = jnp.where(lane_group == a, turned[(a - q) % SUB], piece)
                stage_scr[half * 4 + q, pl.ds(pl.multiple_of(slot * PITCH, 8), groups), :] = piece

    def slot_step(step, carry):
        for u in range(UNROLL):
            slot = step * UNROLL + u
            pltpu.make_async_copy(leg_hbm.at[slot], leg_ref.at[slot], leg_sem.at[slot]).wait()
        for u in range(UNROLL):
            one_slot(step * UNROLL + u)
        return carry

    lax.fori_loop(0, slots // UNROLL, slot_step, 0)

    def emit(dest, carry):
        for third in range(3):
            for q in range(4):
                tiles = [stage_scr[q * 2 + r, pl.ds(dest * 3 + third, 8, stride=PITCH), :] for r in range(2)]
                out_ref[dest, q, third] = jnp.concatenate(tiles, axis=0).astype(BF16)
        return carry

    share = dests // 4

    def emit_part(part, carry):
        lax.fori_loop(part * share, (part + 1) * share, emit, 0)
        here = pl.ds(part * share, share)
        pltpu.make_async_copy(out_ref.at[here], out_hbm.at[here], out_sem.at[part]).start()
        return carry

    lax.fori_loop(0, 4, emit_part, 0)
    for part in range(4):
        here = pl.ds(part * share, share)
        pltpu.make_async_copy(out_ref.at[here], out_hbm.at[here], out_sem.at[part]).wait()


def front(control, vert_root, loc_spec, legendre, lat_order):
    members, levels, _, slots, waves = control.shape
    lats = legendre.shape[2]
    ctrl = control.reshape(members, levels, 2 * slots, waves)
    small = pl.BlockSpec(memory_space=pltpu.VMEM)
    far = pl.BlockSpec(memory_space=pltpu.HBM)
    out = (64, 4, 3, 16, 128)
    return pl.pallas_call(
        front_kernel,
        in_specs=[small, small, small, far, far],
        out_specs=far,
        out_shape=jax.ShapeDtypeStruct(out, BF16),
        scratch_shapes=[
            pltpu.VMEM(ctrl.shape, BF16),
            pltpu.VMEM(legendre.shape, BF16),
            pltpu.VMEM((slots, 256, waves), F32),
            pltpu.VMEM((512, 512), BF16),
            pltpu.VMEM((lats, lats), BF16),
            pltpu.VMEM((8, slots * PITCH, 128), F32),
            pltpu.VMEM(out, BF16),
            pltpu.SemaphoreType.DMA((members,)),
            pltpu.SemaphoreType.DMA((slots,)),
            pltpu.SemaphoreType.DMA((4,)),
        ],
        compiler_params=pltpu.CompilerParams(vmem_limit_bytes=60 * 1024 * 1024),
        name="front",
    )(vert_root, loc_spec.reshape(1, waves), lat_order, ctrl, legendre)


def make_basis(wave_table, lon_count):
    waves = wave_table.reshape(-1, 1, 8, 1)
    longitude = lax.iota(jnp.int32, lon_count)
    phases = waves * longitude % lon_count
    angles = phases.astype(F32) * (2.0 * math.pi / lon_count)
    weights = jnp.where(waves == 0, 1.0, 2.0).astype(F32)
    pair = jnp.concatenate([weights * jnp.cos(angles), -weights * jnp.sin(angles)], axis=1)
    return pair.astype(BF16).reshape(-1, lon_count)


COLS = 256


def back_kernel(recv_ref, basis_ref, ptb_ref, out_ref, turn_scr):
    @pl.when(pl.program_id(0) == 0)
    def _():
        for third in range(3):
            for q in range(4):
                coefs = recv_ref[:, q, third].reshape(1024, 128)
                turn_scr[third, pl.ds(q * 128, 128), :] = jnp.transpose(coefs)

    for third in range(3):
        field = dot(turn_scr[third], basis_ref[...], ((1,), (0,))).astype(BF16).astype(F32)
        field = field.reshape(4, SUB, 4, 8, COLS)
        for a in range(SUB):
            total = None
            for q in range(4):
                for k in range(4):
                    term = field[q, a, k] * ptb_ref[third * SUB + a, q * 4 + k].astype(F32)
                    total = term if total is None else total + term
            out_ref[third * SUB + a] = total.astype(BF16)


def back(recv, basis, perturb):
    lats, members, levels, lons = perturb.shape
    return pl.pallas_call(
        back_kernel,
        grid=(lons // COLS,),
        in_specs=[
            pl.BlockSpec(memory_space=pltpu.VMEM),
            pl.BlockSpec((1024, COLS), lambda c: (0, c)),
            pl.BlockSpec((lats, members, levels, COLS), lambda c: (0, 0, 0, c)),
        ],
        out_specs=pl.BlockSpec((lats, levels, COLS), lambda c: (0, 0, c)),
        out_shape=jax.ShapeDtypeStruct((lats, levels, lons), BF16),
        scratch_shapes=[pltpu.VMEM((3, 512, 1024), BF16)],
        compiler_params=pltpu.CompilerParams(vmem_limit_bytes=48 * 1024 * 1024),
        name="back",
    )(recv, basis, perturb)


def shards(control, vert_root, loc_spec, legendre, wave_table, lat_order, perturb):
    send = front(control, vert_root, loc_spec, legendre, lat_order)
    recv = lax.all_to_all(send.reshape(256, 3, 16, 128), ("rows", "mem"), 0, 0, tiled=True)
    basis = make_basis(wave_table, perturb.shape[3])
    return back(recv.reshape(64, 4, 3, 16, 128), basis, perturb)


def solution(mesh):
    return jax.shard_map(
        shards,
        mesh=mesh,
        in_specs=(
            P("mem", None, None, "rows", None),
            P(),
            P(),
            P("rows", None, None),
            P(),
            P(),
            P("rows", None, "mem", None),
        ),
        out_specs=P("rows", "mem", None),
        check_vma=False,
    )
```

```python
import functools
import math

import jax
import jax.numpy as jnp
from jax import lax
from jax.experimental import pallas as pl
from jax.experimental.pallas import tpu as pltpu
from jax.sharding import Mesh
from jax.sharding import PartitionSpec as P

F32 = jnp.float32
BF16 = jnp.bfloat16
SUB = 4
UNROLL = 2
PITCH = 200
NZ = 8


def dot(a, b, dims):
    return lax.dot_general(a, b, (dims, ((), ())), preferred_element_type=F32)


def front_kernel(z_ref, root_ref, loc_ref, lat_ref, ctrl_hbm, leg_hbm, *rest):
    outs_hbm = rest[:10]
    (ctrl_ref, leg_ref, spec_scr, mix_scr, perm_scr, stage_scr) = rest[10:16]
    out_refs = rest[16:26]
    ctrl_sem, leg_sem, out_sem = rest[26:]
    members = ctrl_ref.shape[0]
    slots, waves, lats = leg_ref.shape
    groups = lats // SUB
    ctrl_in = [pltpu.make_async_copy(ctrl_hbm.at[k], ctrl_ref.at[k], ctrl_sem.at[k]) for k in range(members)]
    leg_in = [pltpu.make_async_copy(leg_hbm.at[s], leg_ref.at[s], leg_sem.at[s]) for s in range(slots)]
    for copy in ctrl_in + leg_in:
        copy.start()

    rows = lax.broadcasted_iota(jnp.int32, (32, 512), 0)
    lanes = lax.broadcasted_iota(jnp.int32, (32, 512), 1)
    pick_v = jnp.where(rows == lanes // 16, 1.0, 0.0).astype(BF16)
    spread = dot(root_ref[...].astype(BF16), pick_v, ((1,), (0,)))

    def mix_rows(h, carry):
        mix_scr[pl.ds(pl.multiple_of(h * 32, 32), 32), :] = jnp.where(lanes % 16 == h, spread, 0.0).astype(BF16)
        return carry

    lax.fori_loop(0, 16, mix_rows, 0)

    lat_row = jnp.broadcast_to(lat_ref[...].reshape(1, lats).astype(F32), (128, lats))
    stage_scr[0, pl.ds(0, lats), :] = jnp.transpose(lat_row)
    cols = lax.broadcasted_iota(jnp.int32, (groups, 128), 1).astype(F32)

    def pick_rows(a, carry):
        wanted = stage_scr[0, pl.ds(a, groups, stride=SUB), :]
        rows = pl.ds(pl.multiple_of(a * groups, 64), groups)
        for c in range(lats // 128):
            hit = jnp.where(cols + 128.0 * c == wanted, 1.0, 0.0).astype(BF16)
            perm_scr[rows, pl.ds(c * 128, 128)] = hit
        return carry

    lax.fori_loop(0, SUB, pick_rows, 0)

    def mix_member(k, carry):
        pltpu.make_async_copy(ctrl_hbm.at[k], ctrl_ref.at[k], ctrl_sem.at[k]).wait()
        mixed = dot(mix_scr[...], ctrl_ref[k].reshape(512, waves), ((1,), (0,))) * loc_ref[...]
        for r in range(2):
            for s in range(slots):
                for q in range(4):
                    src = (r * slots + s) * 32 + q * 8
                    rows = pl.ds(pl.multiple_of(q * 64 + r * 32 + k * 8, 8), 8)
                    spec_scr[s, rows, :] = mixed[src:src + 8]
        return carry

    lax.fori_loop(0, members, mix_member, 0)

    def one_slot(slot):
        spec = spec_scr[slot].astype(BF16)
        fourier = dot(spec, leg_ref[slot], ((1,), (0,))).astype(BF16)
        sorted_rows = dot(perm_scr[...], fourier, ((1,), (1,)))
        lane_group = lax.broadcasted_iota(jnp.int32, (groups, 128), 1) // 32
        for half in range(2):
            parts = [sorted_rows[a * groups:(a + 1) * groups, half * 128:(half + 1) * 128] for a in range(SUB)]
            turned = []
            for d in range(SUB):
                piece = parts[d]
                for p in range(1, SUB):
                    piece = jnp.where(lane_group == p, parts[(p + d) % SUB], piece)
                turned.append(pltpu.roll(piece, 32 * d, 1) if d else piece)
            for q in range(4):
                piece = turned[(0 - q) % SUB]
                for a in range(1, SUB):
                    piece = jnp.where(lane_group == a, turned[(a - q) % SUB], piece)
                stage_scr[half * 4 + q, pl.ds(pl.multiple_of(slot * PITCH, 8), groups), :] = piece

    def slot_step(step, carry):
        for u in range(UNROLL):
            slot = step * UNROLL + u
            pltpu.make_async_copy(leg_hbm.at[slot], leg_ref.at[slot], leg_sem.at[slot]).wait()
        for u in range(UNROLL):
            one_slot(step * UNROLL + u)
        return carry

    lax.fori_loop(0, slots // UNROLL, slot_step, 0)

    def tile(q, dest, third):
        tiles = [stage_scr[q * 2 + r, pl.ds(dest * 3 + third, 8, stride=PITCH), :] for r in range(2)]
        return jnp.concatenate(tiles, axis=0).astype(BF16)

    def send(n):
        return pltpu.make_async_copy(out_refs[n], outs_hbm[n], out_sem.at[n])

    def emit_planes(third, peer, carry):
        for dz in range(NZ):
            dest = (z_ref[0] + dz) % NZ * 8 + peer
            for q in range(4):
                out_refs[7 + third][peer * 4 + q, dz] = tile(q, dest, third)
        return carry

    def emit_hops(peer, carry):
        for dz in range(NZ):
            dest = (z_ref[0] + dz) % NZ * 8 + peer
            for q in range(4):
                out_refs[dz][peer * 4 + q] = tile(q, dest, 0)
        return carry

    for third in (1, 2):
        lax.fori_loop(0, 8, functools.partial(emit_planes, third), 0)
        send(7 + third).start()
    lax.fori_loop(0, 8, emit_hops, 0)
    for dz in range(NZ):
        send(dz).start()
    for n in range(10):
        send(n).wait()


def front(place, control, vert_root, loc_spec, legendre, lat_order):
    members, levels, _, slots, waves = control.shape
    lats = legendre.shape[2]
    ctrl = control.reshape(members, levels, 2 * slots, waves)
    small = pl.BlockSpec(memory_space=pltpu.VMEM)
    far = pl.BlockSpec(memory_space=pltpu.HBM)
    outs = [(32, 16, 128)] * NZ + [(32, NZ, 16, 128)] * 2
    return pl.pallas_call(
        front_kernel,
        in_specs=[pl.BlockSpec(memory_space=pltpu.SMEM), small, small, small, far, far],
        out_specs=[far] * 10,
        out_shape=[jax.ShapeDtypeStruct(out, BF16) for out in outs],
        scratch_shapes=[
            pltpu.VMEM(ctrl.shape, BF16),
            pltpu.VMEM(legendre.shape, BF16),
            pltpu.VMEM((slots, 256, waves), F32),
            pltpu.VMEM((512, 512), BF16),
            pltpu.VMEM((lats, lats), BF16),
            pltpu.VMEM((8, slots * PITCH, 128), F32),
            *[pltpu.VMEM(out, BF16) for out in outs],
            pltpu.SemaphoreType.DMA((members,)),
            pltpu.SemaphoreType.DMA((slots,)),
            pltpu.SemaphoreType.DMA((10,)),
        ],
        compiler_params=pltpu.CompilerParams(vmem_limit_bytes=60 * 1024 * 1024),
        name="front",
    )(place, vert_root, loc_spec.reshape(1, waves), lat_order, ctrl, legendre)


BAND = 64


def basis_kernel(wave_ref, out_ref):
    lons = out_ref.shape[1]
    lanes = lax.broadcasted_iota(jnp.int32, (BAND, 128), 1).astype(F32)
    step = 2.0 * math.pi / lons

    def wrap(count, period):
        return count - period * jnp.floor((count + 0.5) * (1.0 / period))

    def band(i, carry):
        wave = wave_ref[pl.ds(pl.multiple_of(i * BAND, BAND), BAND), :]
        count = wave * lanes
        near = wrap(count, float(lons)) * step
        far = wrap(count, lons / 128.0) * (128.0 * step)
        weight = jnp.where(wave == 0.0, 1.0, 2.0)
        near_cos, near_sin = weight * jnp.cos(near), weight * jnp.sin(near)
        far_cos, far_sin = jnp.cos(far), jnp.sin(far)
        for b in range(lons // 128):
            c, s = far_cos[:, b:b + 1], far_sin[:, b:b + 1]
            real = c * near_cos - s * near_sin
            imag = -(s * near_cos + c * near_sin)
            for row in range(BAND // 8):
                cut = slice(row * 8, row * 8 + 8)
                both = jnp.concatenate([real[cut], imag[cut]], axis=0).astype(BF16)
                out_ref[pl.ds(pl.multiple_of(i * 2 * BAND + row * 16, 16), 16), pl.ds(b * 128, 128)] = both
        return carry

    lax.fori_loop(0, wave_ref.shape[0] // BAND, band, 0)


def make_basis(wave_table, lon_count):
    waves = wave_table.shape[0]
    return pl.pallas_call(
        basis_kernel,
        out_shape=jax.ShapeDtypeStruct((2 * waves, lon_count), BF16),
        compiler_params=pltpu.CompilerParams(vmem_limit_bytes=48 * 1024 * 1024),
        name="basis",
    )(jnp.broadcast_to(wave_table.astype(F32)[:, None], (waves, 128)))


def stack_kernel(*refs):
    for dz in range(NZ):
        refs[NZ][:, dz] = refs[dz][...]


def stack(blocks):
    near = pl.BlockSpec(memory_space=pltpu.VMEM)
    return pl.pallas_call(
        stack_kernel,
        in_specs=[near] * NZ,
        out_specs=near,
        out_shape=jax.ShapeDtypeStruct((32, NZ, 16, 128), BF16),
        compiler_params=pltpu.CompilerParams(vmem_limit_bytes=48 * 1024 * 1024),
        name="stack",
    )(*blocks)


COLS = 512


def back_kernel(*refs, counts):
    total_refs = sum(counts)
    recv_refs, (basis_ref, ptb_ref), (out_ref, turn_scr) = refs[:total_refs], refs[total_refs:total_refs + 2], refs[-2:]

    @pl.when(pl.program_id(0) == 0)
    def _():
        first = 0
        for t, count in enumerate(counts):
            for q in range(4):
                for dz in range(NZ):
                    coefs = recv_refs[first][:, q, dz] if count == 1 else recv_refs[first + dz][:, q]
                    turn_scr[t, pl.ds(q * 128, 128), pl.ds(dz * 128, 128)] = jnp.transpose(coefs.reshape(128, 128))
            first += count

    width = 256
    for c in range(COLS // width):
        cols = pl.ds(c * width, width)
        for t in range(len(counts)):
            field = dot(turn_scr[t], basis_ref[:, cols], ((1,), (0,))).astype(BF16).astype(F32)
            field = field.reshape(4, SUB, 4, 8, width)
            for a in range(SUB):
                total = None
                for q in range(4):
                    for k in range(4):
                        term = field[q, a, k] * ptb_ref[t * SUB + a, q * 4 + k, :, cols].astype(F32)
                        total = term if total is None else total + term
                out_ref[t * SUB + a, :, cols] = total.astype(BF16)


def back(groups, basis, perturb, block, done):
    lats, members, levels, lons = perturb.shape
    counts = tuple(len(pieces) for pieces in groups)
    rows = SUB * len(groups)
    args = []
    for pieces in groups:
        shape = (8, 4, NZ, 16, 128) if len(pieces) == 1 else (8, 4, 16, 128)
        args += [piece.reshape(shape) for piece in pieces]
    specs = [pl.BlockSpec(memory_space=pltpu.VMEM)] * len(args) + [
        pl.BlockSpec((1024, COLS), lambda c: (0, c)),
        pl.BlockSpec((rows, members, levels, COLS), lambda c: (block, 0, 0, c)),
    ]
    args += [basis, perturb]
    aliases = {}
    if done is not None:
        aliases = {len(args): 0}
        specs.append(pl.BlockSpec(memory_space=pl.ANY))
        args.append(done)
    return pl.pallas_call(
        functools.partial(back_kernel, counts=counts),
        grid=(lons // COLS,),
        in_specs=specs,
        out_specs=pl.BlockSpec((rows, levels, COLS), lambda c: (block, 0, c)),
        out_shape=jax.ShapeDtypeStruct((lats, levels, lons), BF16),
        scratch_shapes=[pltpu.VMEM((len(groups), 512, 1024), BF16)],
        input_output_aliases=aliases,
        compiler_params=pltpu.CompilerParams(vmem_limit_bytes=48 * 1024 * 1024),
        name="back",
    )(*args)


def hop(blocks):
    moved = [blocks[0]]
    for dz in range(1, NZ):
        moved.append(lax.ppermute(blocks[dz], "z", [(i, (i + dz) % NZ) for i in range(NZ)]))
    return moved


def planes(block):
    return [block[:, dz] for dz in range(NZ)]


def plane(block):
    return lax.all_to_all(block, ("y", "c", "mem"), 0, 0, tiled=True)


def shards(control, vert_root, loc_spec, legendre, wave_table, lat_order, perturb):
    place = lax.axis_index("z")
    sends = front(place.reshape(1), control, vert_root, loc_spec, legendre, lat_order)
    table = jnp.roll(jnp.flip(wave_table.reshape(NZ, -1), 0), place + 1, 0)
    basis = make_basis(table.reshape(-1), perturb.shape[3])
    one = plane(sends[8])
    zero = hop(sends[:8])
    two = plane(sends[9])
    one = hop(planes(one))
    two = hop(planes(two))
    zero = stack(zero)
    zero = plane(zero)
    done = back([[zero], one], basis, perturb, 0, None)
    return back([two], basis, perturb, 2, done)


def solution(mesh):
    split = Mesh(mesh.devices.reshape(NZ, 4, 2, 4), ("z", "y", "c", "mem"))
    rows = ("z", "y", "c")
    return jax.shard_map(
        shards,
        mesh=split,
        in_specs=(
            P("mem", None, None, rows, None),
            P(),
            P(),
            P(rows, None, None),
            P(),
            P(),
            P(rows, None, "mem", None),
        ),
        out_specs=P(rows, "mem", None),
        check_vma=False,
    )
```

```python
import functools
import math

import jax
import jax.numpy as jnp
from jax import lax
from jax.experimental import pallas as pl
from jax.experimental.pallas import tpu as pltpu
from jax.sharding import Mesh
from jax.sharding import PartitionSpec as P

F32 = jnp.float32
BF16 = jnp.bfloat16
SUB = 4
UNROLL = 2
PITCH = 200
NZ = 8


def dot(a, b, dims):
    return lax.dot_general(a, b, (dims, ((), ())), preferred_element_type=F32)


def front_kernel(z_ref, root_ref, loc_ref, lat_ref, ctrl_hbm, leg_hbm, *rest):
    outs_hbm = rest[:10]
    (ctrl_ref, leg_ref, spec_scr, mix_scr, perm_scr, stage_scr) = rest[10:16]
    out_refs = rest[16:26]
    ctrl_sem, leg_sem, out_sem = rest[26:]
    members = ctrl_ref.shape[0]
    slots, waves, lats = leg_ref.shape
    groups = lats // SUB
    ctrl_in = [pltpu.make_async_copy(ctrl_hbm.at[k], ctrl_ref.at[k], ctrl_sem.at[k]) for k in range(members)]
    leg_in = [pltpu.make_async_copy(leg_hbm.at[s], leg_ref.at[s], leg_sem.at[s]) for s in range(slots)]
    for copy in ctrl_in + leg_in:
        copy.start()

    rows = lax.broadcasted_iota(jnp.int32, (32, 512), 0)
    lanes = lax.broadcasted_iota(jnp.int32, (32, 512), 1)
    pick_v = jnp.where(rows == lanes // 16, 1.0, 0.0).astype(BF16)
    spread = dot(root_ref[...].astype(BF16), pick_v, ((1,), (0,)))

    def mix_rows(h, carry):
        mix_scr[pl.ds(pl.multiple_of(h * 32, 32), 32), :] = jnp.where(lanes % 16 == h, spread, 0.0).astype(BF16)
        return carry

    lax.fori_loop(0, 16, mix_rows, 0)

    lat_row = jnp.broadcast_to(lat_ref[...].reshape(1, lats).astype(F32), (128, lats))
    stage_scr[0, pl.ds(0, lats), :] = jnp.transpose(lat_row)
    cols = lax.broadcasted_iota(jnp.int32, (groups, 128), 1).astype(F32)

    def pick_rows(a, carry):
        wanted = stage_scr[0, pl.ds(a, groups, stride=SUB), :]
        rows = pl.ds(pl.multiple_of(a * groups, 64), groups)
        for c in range(lats // 128):
            hit = jnp.where(cols + 128.0 * c == wanted, 1.0, 0.0).astype(BF16)
            perm_scr[rows, pl.ds(c * 128, 128)] = hit
        return carry

    lax.fori_loop(0, SUB, pick_rows, 0)

    def mix_member(k, carry):
        pltpu.make_async_copy(ctrl_hbm.at[k], ctrl_ref.at[k], ctrl_sem.at[k]).wait()
        mixed = dot(mix_scr[...], ctrl_ref[k].reshape(512, waves), ((1,), (0,))) * loc_ref[...]
        for r in range(2):
            for s in range(slots):
                for q in range(4):
                    src = (r * slots + s) * 32 + q * 8
                    rows = pl.ds(pl.multiple_of(q * 64 + r * 32 + k * 8, 8), 8)
                    spec_scr[s, rows, :] = mixed[src:src + 8]
        return carry

    lax.fori_loop(0, members, mix_member, 0)

    def one_slot(slot):
        spec = spec_scr[slot].astype(BF16)
        fourier = dot(spec, leg_ref[slot], ((1,), (0,))).astype(BF16)
        sorted_rows = dot(perm_scr[...], fourier, ((1,), (1,)))
        lane_group = lax.broadcasted_iota(jnp.int32, (groups, 128), 1) // 32
        for half in range(2):
            parts = [sorted_rows[a * groups:(a + 1) * groups, half * 128:(half + 1) * 128] for a in range(SUB)]
            turned = []
            for d in range(SUB):
                piece = parts[d]
                for p in range(1, SUB):
                    piece = jnp.where(lane_group == p, parts[(p + d) % SUB], piece)
                turned.append(pltpu.roll(piece, 32 * d, 1) if d else piece)
            for q in range(4):
                piece = turned[(0 - q) % SUB]
                for a in range(1, SUB):
                    piece = jnp.where(lane_group == a, turned[(a - q) % SUB], piece)
                stage_scr[half * 4 + q, pl.ds(pl.multiple_of(slot * PITCH, 8), groups), :] = piece

    def slot_step(step, carry):
        for u in range(UNROLL):
            slot = step * UNROLL + u
            pltpu.make_async_copy(leg_hbm.at[slot], leg_ref.at[slot], leg_sem.at[slot]).wait()
        for u in range(UNROLL):
            one_slot(step * UNROLL + u)
        return carry

    lax.fori_loop(0, slots // UNROLL, slot_step, 0)

    def tile(q, dest, third):
        tiles = [stage_scr[q * 2 + r, pl.ds(dest * 3 + third, 8, stride=PITCH), :] for r in range(2)]
        return jnp.concatenate(tiles, axis=0).astype(BF16)

    def send(n):
        return pltpu.make_async_copy(out_refs[n], outs_hbm[n], out_sem.at[n])

    def emit_planes(third, peer, carry):
        for dz in range(NZ):
            dest = (z_ref[0] + dz) % NZ * 8 + peer
            for q in range(4):
                out_refs[7 + third][peer * 4 + q, dz] = tile(q, dest, third)
        return carry

    def emit_hops(peer, carry):
        for dz in range(NZ):
            dest = (z_ref[0] + dz) % NZ * 8 + peer
            for q in range(4):
                out_refs[dz][peer * 4 + q] = tile(q, dest, 0)
        return carry

    for third in (1, 2):
        lax.fori_loop(0, 8, functools.partial(emit_planes, third), 0)
        send(7 + third).start()
    lax.fori_loop(0, 8, emit_hops, 0)
    for dz in range(NZ):
        send(dz).start()
    for n in range(10):
        send(n).wait()


def front(place, control, vert_root, loc_spec, legendre, lat_order):
    members, levels, _, slots, waves = control.shape
    lats = legendre.shape[2]
    ctrl = control.reshape(members, levels, 2 * slots, waves)
    small = pl.BlockSpec(memory_space=pltpu.VMEM)
    far = pl.BlockSpec(memory_space=pltpu.HBM)
    outs = [(32, 16, 128)] * NZ + [(32, NZ, 16, 128)] * 2
    return pl.pallas_call(
        front_kernel,
        in_specs=[pl.BlockSpec(memory_space=pltpu.SMEM), small, small, small, far, far],
        out_specs=[far] * 10,
        out_shape=[jax.ShapeDtypeStruct(out, BF16) for out in outs],
        scratch_shapes=[
            pltpu.VMEM(ctrl.shape, BF16),
            pltpu.VMEM(legendre.shape, BF16),
            pltpu.VMEM((slots, 256, waves), F32),
            pltpu.VMEM((512, 512), BF16),
            pltpu.VMEM((lats, lats), BF16),
            pltpu.VMEM((8, (slots + 1) * PITCH, 128), F32),
            *[pltpu.VMEM(out, BF16) for out in outs],
            pltpu.SemaphoreType.DMA((members,)),
            pltpu.SemaphoreType.DMA((slots,)),
            pltpu.SemaphoreType.DMA((10,)),
        ],
        compiler_params=pltpu.CompilerParams(vmem_limit_bytes=60 * 1024 * 1024),
        name="front",
    )(place, vert_root, loc_spec.reshape(1, waves), lat_order, ctrl, legendre)


BAND = 64


def basis_kernel(wave_ref, out_ref):
    lons = out_ref.shape[1]
    lanes = lax.broadcasted_iota(jnp.int32, (BAND, 128), 1).astype(F32)

    def turns(count, period):
        return count - period * jnp.floor((count + 0.5) * (1.0 / period) + 0.5)

    def circle(part):
        half = part * math.pi
        sq = half * half
        sin_half = 0.0
        for n in (13, 11, 9, 7, 5, 3, 1):
            sin_half = sin_half * sq + (-1.0) ** (n // 2) / math.factorial(n)
        sin_half = sin_half * half
        cos_half = 0.0
        for n in (12, 10, 8, 6, 4, 2, 0):
            cos_half = cos_half * sq + (-1.0) ** (n // 2) / math.factorial(n)
        return 1.0 - 2.0 * sin_half * sin_half, 2.0 * sin_half * cos_half

    def band(i, carry):
        wave = wave_ref[pl.ds(pl.multiple_of(i * BAND, BAND), BAND), :]
        count = wave * lanes
        near_cos, near_sin = circle(turns(count, float(lons)) * (1.0 / lons))
        far_cos, far_sin = circle(turns(count, lons / 128.0) * (128.0 / lons))
        weight = jnp.where(wave == 0.0, 1.0, 2.0)
        near_cos, near_sin = weight * near_cos, weight * near_sin
        for b in range(lons // 128):
            c, s = far_cos[:, b:b + 1], far_sin[:, b:b + 1]
            real = c * near_cos - s * near_sin
            imag = -(s * near_cos + c * near_sin)
            for row in range(BAND // 8):
                cut = slice(row * 8, row * 8 + 8)
                both = jnp.concatenate([real[cut], imag[cut]], axis=0).astype(BF16)
                out_ref[pl.ds(pl.multiple_of(i * 2 * BAND + row * 16, 16), 16), pl.ds(b * 128, 128)] = both
        return carry

    lax.fori_loop(0, wave_ref.shape[0] // BAND, band, 0)


def make_basis(wave_table, lon_count):
    waves = wave_table.shape[0]
    return pl.pallas_call(
        basis_kernel,
        out_shape=jax.ShapeDtypeStruct((2 * waves, lon_count), BF16),
        compiler_params=pltpu.CompilerParams(vmem_limit_bytes=48 * 1024 * 1024),
        name="basis",
    )(jnp.broadcast_to(wave_table.astype(F32)[:, None], (waves, 128)))


def stack_kernel(*refs):
    for dz in range(NZ):
        refs[NZ][:, dz] = refs[dz][...]


def stack(blocks):
    near = pl.BlockSpec(memory_space=pltpu.VMEM)
    return pl.pallas_call(
        stack_kernel,
        in_specs=[near] * NZ,
        out_specs=near,
        out_shape=jax.ShapeDtypeStruct((32, NZ, 16, 128), BF16),
        compiler_params=pltpu.CompilerParams(vmem_limit_bytes=48 * 1024 * 1024),
        name="stack",
    )(*blocks)


COLS = 512


def back_kernel(*refs, counts):
    total_refs = sum(counts)
    recv_refs, (basis_ref, ptb_ref), (out_ref, turn_scr) = refs[:total_refs], refs[total_refs:total_refs + 2], refs[-2:]

    @pl.when(pl.program_id(0) == 0)
    def _():
        first = 0
        for t, count in enumerate(counts):
            for q in range(4):
                for dz in range(NZ):
                    coefs = recv_refs[first][:, q, dz] if count == 1 else recv_refs[first + dz][:, q]
                    turn_scr[t, pl.ds(q * 128, 128), pl.ds(dz * 128, 128)] = jnp.transpose(coefs.reshape(128, 128))
            first += count

    width = 256
    for c in range(COLS // width):
        cols = pl.ds(c * width, width)
        for t in range(len(counts)):
            field = dot(turn_scr[t], basis_ref[:, cols], ((1,), (0,))).astype(BF16).astype(F32)
            field = field.reshape(4, SUB, 4, 8, width)
            for a in range(SUB):
                total = None
                for q in range(4):
                    for k in range(4):
                        term = field[q, a, k] * ptb_ref[t * SUB + a, q * 4 + k, :, cols].astype(F32)
                        total = term if total is None else total + term
                out_ref[t * SUB + a, :, cols] = total.astype(BF16)


def back(groups, basis, perturb, block, done):
    lats, members, levels, lons = perturb.shape
    counts = tuple(len(pieces) for pieces in groups)
    rows = SUB * len(groups)
    args = []
    for pieces in groups:
        shape = (8, 4, NZ, 16, 128) if len(pieces) == 1 else (8, 4, 16, 128)
        args += [piece.reshape(shape) for piece in pieces]
    specs = [pl.BlockSpec(memory_space=pltpu.VMEM)] * len(args) + [
        pl.BlockSpec((1024, COLS), lambda c: (0, c)),
        pl.BlockSpec((rows, members, levels, COLS), lambda c: (block, 0, 0, c)),
    ]
    args += [basis, perturb]
    aliases = {}
    if done is not None:
        aliases = {len(args): 0}
        specs.append(pl.BlockSpec(memory_space=pl.ANY))
        args.append(done)
    return pl.pallas_call(
        functools.partial(back_kernel, counts=counts),
        grid=(lons // COLS,),
        in_specs=specs,
        out_specs=pl.BlockSpec((rows, levels, COLS), lambda c: (block, 0, c)),
        out_shape=jax.ShapeDtypeStruct((lats, levels, lons), BF16),
        scratch_shapes=[pltpu.VMEM((len(groups), 512, 1024), BF16)],
        input_output_aliases=aliases,
        compiler_params=pltpu.CompilerParams(vmem_limit_bytes=48 * 1024 * 1024),
        name="back",
    )(*args)


def hop(blocks):
    moved = [blocks[0]]
    for dz in range(1, NZ):
        moved.append(lax.ppermute(blocks[dz], "z", [(i, (i + dz) % NZ) for i in range(NZ)]))
    return moved


def planes(block):
    return [block[:, dz] for dz in range(NZ)]


def plane(block):
    return lax.all_to_all(block, ("y", "c", "mem"), 0, 0, tiled=True)


def shards(control, vert_root, loc_spec, legendre, wave_table, lat_order, perturb):
    place = lax.axis_index("z")
    sends = front(place.reshape(1), control, vert_root, loc_spec, legendre, lat_order)
    table = jnp.roll(jnp.flip(wave_table.reshape(NZ, -1), 0), place + 1, 0)
    basis = make_basis(table.reshape(-1), perturb.shape[3])
    one = plane(sends[8])
    zero = hop(sends[:8])
    two = plane(sends[9])
    one = hop(planes(one))
    two = hop(planes(two))
    zero = stack(zero)
    zero = plane(zero)
    done = back([[zero], one], basis, perturb, 0, None)
    return back([two], basis, perturb, 2, done)


def solution(mesh):
    split = Mesh(mesh.devices.reshape(NZ, 4, 2, 4), ("z", "y", "c", "mem"))
    rows = ("z", "y", "c")
    return jax.shard_map(
        shards,
        mesh=split,
        in_specs=(
            P("mem", None, None, rows, None),
            P(),
            P(),
            P(rows, None, None),
            P(),
            P(),
            P(rows, None, "mem", None),
        ),
        out_specs=P(rows, "mem", None),
        check_vma=False,
    )
```

```python
import functools
import math

import jax
import jax.numpy as jnp
from jax import lax
from jax.experimental import pallas as pl
from jax.experimental.pallas import tpu as pltpu
from jax.sharding import Mesh
from jax.sharding import PartitionSpec as P

F32 = jnp.float32
BF16 = jnp.bfloat16
SUB = 4
UNROLL = 2
PITCH = 200
NZ = 8


def dot(a, b, dims):
    return lax.dot_general(a, b, (dims, ((), ())), preferred_element_type=F32)


def front_kernel(z_ref, root_ref, loc_ref, lat_ref, ctrl_hbm, leg_hbm, *rest):
    outs_hbm = rest[:10]
    (ctrl_ref, leg_ref, spec_scr, mix_scr, perm_scr, stage_scr) = rest[10:16]
    out_refs = rest[16:26]
    ctrl_sem, leg_sem, out_sem = rest[26:]
    members = ctrl_ref.shape[0]
    slots, waves, lats = leg_ref.shape
    groups = lats // SUB
    ctrl_in = [pltpu.make_async_copy(ctrl_hbm.at[k], ctrl_ref.at[k], ctrl_sem.at[k]) for k in range(members)]
    leg_in = [pltpu.make_async_copy(leg_hbm.at[s], leg_ref.at[s], leg_sem.at[s]) for s in range(slots)]
    for copy in ctrl_in + leg_in:
        copy.start()

    rows = lax.broadcasted_iota(jnp.int32, (32, 512), 0)
    lanes = lax.broadcasted_iota(jnp.int32, (32, 512), 1)
    pick_v = jnp.where(rows == lanes // 16, 1.0, 0.0).astype(BF16)
    spread = dot(root_ref[...].astype(BF16), pick_v, ((1,), (0,)))

    def mix_rows(h, carry):
        mix_scr[pl.ds(pl.multiple_of(h * 32, 32), 32), :] = jnp.where(lanes % 16 == h, spread, 0.0).astype(BF16)
        return carry

    lax.fori_loop(0, 16, mix_rows, 0)

    lat_row = jnp.broadcast_to(lat_ref[...].reshape(1, lats).astype(F32), (128, lats))
    stage_scr[0, pl.ds(0, lats), :] = jnp.transpose(lat_row)
    cols = lax.broadcasted_iota(jnp.int32, (groups, 128), 1).astype(F32)

    def pick_rows(a, carry):
        wanted = stage_scr[0, pl.ds(a, groups, stride=SUB), :]
        rows = pl.ds(pl.multiple_of(a * groups, 64), groups)
        for c in range(lats // 128):
            hit = jnp.where(cols + 128.0 * c == wanted, 1.0, 0.0).astype(BF16)
            perm_scr[rows, pl.ds(c * 128, 128)] = hit
        return carry

    lax.fori_loop(0, SUB, pick_rows, 0)

    def mix_member(k, carry):
        pltpu.make_async_copy(ctrl_hbm.at[k], ctrl_ref.at[k], ctrl_sem.at[k]).wait()
        mixed = dot(mix_scr[...], ctrl_ref[k].reshape(512, waves), ((1,), (0,))) * loc_ref[...]
        for r in range(2):
            for s in range(slots):
                for q in range(4):
                    src = (r * slots + s) * 32 + q * 8
                    rows = pl.ds(pl.multiple_of(q * 64 + r * 32 + k * 8, 8), 8)
                    spec_scr[s, rows, :] = mixed[src:src + 8]
        return carry

    lax.fori_loop(0, members, mix_member, 0)

    def one_slot(slot):
        spec = spec_scr[slot].astype(BF16)
        fourier = dot(spec, leg_ref[slot], ((1,), (0,))).astype(BF16)
        sorted_rows = dot(perm_scr[...], fourier, ((1,), (1,)))
        lane_group = lax.broadcasted_iota(jnp.int32, (groups, 128), 1) // 32
        for half in range(2):
            parts = [sorted_rows[a * groups:(a + 1) * groups, half * 128:(half + 1) * 128] for a in range(SUB)]
            turned = []
            for d in range(SUB):
                piece = parts[d]
                for p in range(1, SUB):
                    piece = jnp.where(lane_group == p, parts[(p + d) % SUB], piece)
                turned.append(pltpu.roll(piece, 32 * d, 1) if d else piece)
            for q in range(4):
                piece = turned[(0 - q) % SUB]
                for a in range(1, SUB):
                    piece = jnp.where(lane_group == a, turned[(a - q) % SUB], piece)
                stage_scr[half * 4 + q, pl.ds(pl.multiple_of(slot * PITCH, 8), groups), :] = piece

    def slot_step(step, carry):
        for u in range(UNROLL):
            slot = step * UNROLL + u
            pltpu.make_async_copy(leg_hbm.at[slot], leg_ref.at[slot], leg_sem.at[slot]).wait()
        for u in range(UNROLL):
            one_slot(step * UNROLL + u)
        return carry

    lax.fori_loop(0, slots // UNROLL, slot_step, 0)

    def tile(q, dest, third):
        tiles = [stage_scr[q * 2 + r, pl.ds(dest * 3 + third, 8, stride=PITCH), :] for r in range(2)]
        return jnp.concatenate(tiles, axis=0).astype(BF16)

    def send(n):
        return pltpu.make_async_copy(out_refs[n], outs_hbm[n], out_sem.at[n])

    def emit_planes(third, peer, carry):
        for dz in range(NZ):
            dest = (z_ref[0] + dz) % NZ * 8 + peer
            for q in range(4):
                out_refs[7 + third][peer * 4 + q, dz] = tile(q, dest, third)
        return carry

    def emit_hops(peer, carry):
        for dz in range(NZ):
            dest = (z_ref[0] + dz) % NZ * 8 + peer
            for q in range(4):
                out_refs[dz][peer * 4 + q] = tile(q, dest, 0)
        return carry

    for third in (1, 2):
        lax.fori_loop(0, 8, functools.partial(emit_planes, third), 0)
        send(7 + third).start()
    lax.fori_loop(0, 8, emit_hops, 0)
    for dz in range(NZ):
        send(dz).start()
    for n in range(10):
        send(n).wait()


def front(place, control, vert_root, loc_spec, legendre, lat_order):
    members, levels, _, slots, waves = control.shape
    lats = legendre.shape[2]
    ctrl = control.reshape(members, levels, 2 * slots, waves)
    small = pl.BlockSpec(memory_space=pltpu.VMEM)
    far = pl.BlockSpec(memory_space=pltpu.HBM)
    outs = [(32, 16, 128)] * NZ + [(32, NZ, 16, 128)] * 2
    return pl.pallas_call(
        front_kernel,
        in_specs=[pl.BlockSpec(memory_space=pltpu.SMEM), small, small, small, far, far],
        out_specs=[far] * 10,
        out_shape=[jax.ShapeDtypeStruct(out, BF16) for out in outs],
        scratch_shapes=[
            pltpu.VMEM(ctrl.shape, BF16),
            pltpu.VMEM(legendre.shape, BF16),
            pltpu.VMEM((slots, 256, waves), F32),
            pltpu.VMEM((512, 512), BF16),
            pltpu.VMEM((lats, lats), BF16),
            pltpu.VMEM((8, (slots + 1) * PITCH, 128), F32),
            *[pltpu.VMEM(out, BF16) for out in outs],
            pltpu.SemaphoreType.DMA((members,)),
            pltpu.SemaphoreType.DMA((slots,)),
            pltpu.SemaphoreType.DMA((10,)),
        ],
        compiler_params=pltpu.CompilerParams(vmem_limit_bytes=60 * 1024 * 1024),
        name="front",
    )(place, vert_root, loc_spec.reshape(1, waves), lat_order, ctrl, legendre)


BAND = 64


def basis_kernel(wave_ref, out_ref):
    lons = out_ref.shape[1]
    lanes = lax.broadcasted_iota(jnp.int32, (BAND, 128), 1).astype(F32)

    def turns(count, period):
        return count - period * jnp.floor((count + 0.5) * (1.0 / period) + 0.5)

    def circle(part):
        half = part * math.pi
        sq = half * half
        sin_half = 0.0
        for n in (13, 11, 9, 7, 5, 3, 1):
            sin_half = sin_half * sq + (-1.0) ** (n // 2) / math.factorial(n)
        sin_half = sin_half * half
        cos_half = 0.0
        for n in (12, 10, 8, 6, 4, 2, 0):
            cos_half = cos_half * sq + (-1.0) ** (n // 2) / math.factorial(n)
        return 1.0 - 2.0 * sin_half * sin_half, 2.0 * sin_half * cos_half

    def band(i, carry):
        wave = wave_ref[pl.ds(pl.multiple_of(i * BAND, BAND), BAND), :]
        count = wave * lanes
        near_cos, near_sin = circle(turns(count, float(lons)) * (1.0 / lons))
        far_cos, far_sin = circle(turns(count, lons / 128.0) * (128.0 / lons))
        weight = jnp.where(wave == 0.0, 1.0, 2.0)
        near_cos, near_sin = weight * near_cos, weight * near_sin
        flip = 1.0 - 2.0 * (wave - 2.0 * jnp.floor(wave * 0.5))
        blocks = lons // 256
        for b in range(blocks):
            c, s = far_cos[:, b:b + 1], far_sin[:, b:b + 1]
            real = c * near_cos - s * near_sin
            imag = -(s * near_cos + c * near_sin)
            for shift, (first, second) in enumerate(((real, imag), (real * flip, imag * flip))):
                cols = pl.ds((b + shift * blocks) * 128, 128)
                for row in range(BAND // 8):
                    cut = slice(row * 8, row * 8 + 8)
                    both = jnp.concatenate([first[cut], second[cut]], axis=0).astype(BF16)
                    out_ref[pl.ds(pl.multiple_of(i * 2 * BAND + row * 16, 16), 16), cols] = both
        return carry

    lax.fori_loop(0, wave_ref.shape[0] // BAND, band, 0)


def make_basis(wave_table, lon_count):
    waves = wave_table.shape[0]
    return pl.pallas_call(
        basis_kernel,
        out_shape=jax.ShapeDtypeStruct((2 * waves, lon_count), BF16),
        compiler_params=pltpu.CompilerParams(vmem_limit_bytes=48 * 1024 * 1024),
        name="basis",
    )(jnp.broadcast_to(wave_table.astype(F32)[:, None], (waves, 128)))


def stack_kernel(*refs):
    for dz in range(NZ):
        refs[NZ][:, dz] = refs[dz][...]


def stack(blocks):
    near = pl.BlockSpec(memory_space=pltpu.VMEM)
    return pl.pallas_call(
        stack_kernel,
        in_specs=[near] * NZ,
        out_specs=near,
        out_shape=jax.ShapeDtypeStruct((32, NZ, 16, 128), BF16),
        compiler_params=pltpu.CompilerParams(vmem_limit_bytes=48 * 1024 * 1024),
        name="stack",
    )(*blocks)


COLS = 512


def back_kernel(*refs, counts):
    total_refs = sum(counts)
    recv_refs, (basis_ref, ptb_ref), (out_ref, turn_scr) = refs[:total_refs], refs[total_refs:total_refs + 2], refs[-2:]

    @pl.when(pl.program_id(0) == 0)
    def _():
        first = 0
        for t, count in enumerate(counts):
            for q in range(4):
                for dz in range(NZ):
                    coefs = recv_refs[first][:, q, dz] if count == 1 else recv_refs[first + dz][:, q]
                    turn_scr[t, pl.ds(q * 128, 128), pl.ds(dz * 128, 128)] = jnp.transpose(coefs.reshape(128, 128))
            first += count

    width = 256
    for c in range(COLS // width):
        cols = pl.ds(c * width, width)
        for t in range(len(counts)):
            field = dot(turn_scr[t], basis_ref[:, cols], ((1,), (0,))).astype(BF16).astype(F32)
            field = field.reshape(4, SUB, 4, 8, width)
            for a in range(SUB):
                total = None
                for q in range(4):
                    for k in range(4):
                        term = field[q, a, k] * ptb_ref[t * SUB + a, q * 4 + k, :, cols].astype(F32)
                        total = term if total is None else total + term
                out_ref[t * SUB + a, :, cols] = total.astype(BF16)


def back(groups, basis, perturb, block, done):
    lats, members, levels, lons = perturb.shape
    counts = tuple(len(pieces) for pieces in groups)
    rows = SUB * len(groups)
    args = []
    for pieces in groups:
        shape = (8, 4, NZ, 16, 128) if len(pieces) == 1 else (8, 4, 16, 128)
        args += [piece.reshape(shape) for piece in pieces]
    specs = [pl.BlockSpec(memory_space=pltpu.VMEM)] * len(args) + [
        pl.BlockSpec((1024, COLS), lambda c: (0, c)),
        pl.BlockSpec((rows, members, levels, COLS), lambda c: (block, 0, 0, c)),
    ]
    args += [basis, perturb]
    aliases = {}
    if done is not None:
        aliases = {len(args): 0}
        specs.append(pl.BlockSpec(memory_space=pl.ANY))
        args.append(done)
    return pl.pallas_call(
        functools.partial(back_kernel, counts=counts),
        grid=(lons // COLS,),
        in_specs=specs,
        out_specs=pl.BlockSpec((rows, levels, COLS), lambda c: (block, 0, c)),
        out_shape=jax.ShapeDtypeStruct((lats, levels, lons), BF16),
        scratch_shapes=[pltpu.VMEM((len(groups), 512, 1024), BF16)],
        input_output_aliases=aliases,
        compiler_params=pltpu.CompilerParams(vmem_limit_bytes=48 * 1024 * 1024),
        name="back",
    )(*args)


def hop(blocks):
    moved = [blocks[0]]
    for dz in range(1, NZ):
        moved.append(lax.ppermute(blocks[dz], "z", [(i, (i + dz) % NZ) for i in range(NZ)]))
    return moved


def planes(block):
    return [block[:, dz] for dz in range(NZ)]


def plane(block):
    return lax.all_to_all(block, ("y", "c", "mem"), 0, 0, tiled=True)


def shards(control, vert_root, loc_spec, legendre, wave_table, lat_order, perturb):
    place = lax.axis_index("z")
    sends = front(place.reshape(1), control, vert_root, loc_spec, legendre, lat_order)
    table = jnp.roll(jnp.flip(wave_table.reshape(NZ, -1), 0), place + 1, 0)
    basis = make_basis(table.reshape(-1), perturb.shape[3])
    one = plane(sends[8])
    zero = hop(sends[:8])
    two = plane(sends[9])
    one = hop(planes(one))
    two = hop(planes(two))
    zero = stack(zero)
    zero = plane(zero)
    done = back([[zero], one], basis, perturb, 0, None)
    return back([two], basis, perturb, 2, done)


def solution(mesh):
    split = Mesh(mesh.devices.reshape(NZ, 4, 2, 4), ("z", "y", "c", "mem"))
    rows = ("z", "y", "c")
    return jax.shard_map(
        shards,
        mesh=split,
        in_specs=(
            P("mem", None, None, rows, None),
            P(),
            P(),
            P(rows, None, None),
            P(),
            P(),
            P(rows, None, "mem", None),
        ),
        out_specs=P(rows, "mem", None),
        check_vma=False,
    )
```
